32 devices in a mesh: dp: 8 (over z, y), head: 4 (over x, core).
Axes of the slice: x: 2, y: 2, z: 4, core: 2. Of those that a mesh axis runs over, the one named last changes fastest.
Arguments:
- tokens: bfloat16 [8, 6312, 768], P('dp', 'head'), may hold values from -6 to 6
- frames: int32 [8], P('dp'), may hold values from 4 to 16
- text_mask: int32 [8, 40], P('dp'), may hold values 0 or 1
- latents: bfloat16 [8, 128, 768], P('dp'), may hold values from -6 to 6
- cross_q: bfloat16 [768, 768], P('head'), may hold values from -0.21875 to 0.21875
- cross_kv: bfloat16 [2, 768, 768], P(None, 'head'), may hold values from -0.21875 to 0.21875
- cross_out: bfloat16 [768, 768], P('head'), may hold values from -3.5 to 3.5
- cross_up: bfloat16 [768, 3072], P(None, 'head'), may hold values from -0.21875 to 0.21875
- cross_down: bfloat16 [3072, 768], P('head'), may hold values from -0.109375 to 0.109375
- self_qkv: bfloat16 [3, 768, 768], P(None, 'head'), may hold values from -0.21875 to 0.21875
- self_out: bfloat16 [768, 768], P('head'), may hold values from -0.875 to 0.875
- self_up: bfloat16 [768, 3072], P(None, 'head'), may hold values from -0.21875 to 0.21875
- self_down: bfloat16 [3072, 768], P('head'), may hold values from -0.109375 to 0.109375
- head_bias: float32 [2, 2, 768], P(None, None, 'head'), may hold values from -1.8 to 1.8
- up_bias: float32 [2, 3072], P(None, 'head'), may hold values from -1.8 to 1.8
- out_bias: float32 [2, 2, 768], replicated, may hold values from -1.8 to 1.8
- norm_gain: float32 [5, 768], replicated, may hold values from 0.5 to 1.5
- norm_bias: float32 [5, 768], replicated, may hold values from -1.8 to 1.8
- latents_cot: float32 [8, 128, 768], P('dp'), may hold values from -6 to 6
Outputs:
- latents_out: float32 [8, 128, 768], P('dp')
- grad_tokens: bfloat16 [8, 6312, 768], P('dp', 'head')
- grad_latents: float32 [8, 128, 768], P('dp')
- grad_cross_q: float32 [768, 768], P('head', 'dp')
- grad_cross_kv: float32 [2, 768, 768], P(None, 'head', 'dp')
- grad_cross_out: float32 [768, 768], P('head', 'dp')
- grad_cross_up: float32 [768, 3072], P('dp', 'head')
- grad_cross_down: float32 [3072, 768], P('head', 'dp')
- grad_self_qkv: float32 [3, 768, 768], P(None, 'head', 'dp')
- grad_self_out: float32 [768, 768], P('head', 'dp')
- grad_self_up: float32 [768, 3072], P('dp', 'head')
- grad_self_down: float32 [3072, 768], P('head', 'dp')
- grad_head_bias: float32 [2, 2, 768], P(None, None, 'head')
- grad_up_bias: float32 [2, 3072], P(None, 'head')
- grad_out_bias: float32 [2, 2, 768], P(None, None, 'head')
- grad_norm_gain: float32 [5, 768], P(None, 'head')
- grad_norm_bias: float32 [5, 768], P(None, 'head')
The draws below stay inside these ranges and needn't reach their ends.
Inputs may be any that keep to these rules, and one draw needn't show every extreme that they name: The patches of frames at or after frames[c] are padding.
All inputs are finite; a program needn't handle non-finite values. No bound on the sum of `text_mask` on one device may be relied on, other than what follows from the above.
Results may differ from the reference program's by a relative error of at most 0.018.
Values may be sent and summed in bfloat16 or wider, within the bound.
A program may use at most 128 MiB of HBM per device.

```python
import jax
import jax.numpy as jnp
from jax import lax

D = 768
HEADS = 12
HD = 64
FF = 3072
NL = 128
P_SIZE = 392
TXT = 40
F_MAX = 16
F_MIN = 4
CLIPS = 8
LEN = 6312


def set_ends(values, own_key, least, largest):
    place = [jax.random.randint(jax.random.fold_in(own_key, axis), (), 0, length) for axis, length in enumerate(values.shape)]
    widest = values.shape.index(max(values.shape))
    beside = place[:widest] + [(place[widest] + 1) % values.shape[widest]] + place[widest + 1:]
    return values.at[tuple(place)].set(least).at[tuple(beside)].set(largest)


def block_scale(stream_key, extent, cuts, least, top_value):
    gain = 1.0
    for dim, parts in cuts:
        draws = jax.random.uniform(jax.random.fold_in(jax.random.fold_in(stream_key, 6), dim), (parts,), jnp.float32, least / len(cuts), top_value / len(cuts))
        gain = gain * jnp.repeat(jnp.exp(draws), extent[dim] // parts).reshape((-1,) + (1,) * (len(extent) - 1 - dim))
    return gain


def noise(own_key, extent, width, most, split=(), kind=jnp.bfloat16):
    factor_of = block_scale(own_key, extent, split, -0.22, 0.18) if split else 1.0
    values = jax.random.normal(own_key, extent, jnp.float32) * width * factor_of
    return jnp.minimum(jnp.maximum(values, -most), most).astype(kind)


def setup_inputs(seed: int = 0) -> dict:
    streams_of = jax.random.split(jax.random.key(seed), 20)
    tokens = noise(streams_of[0], (CLIPS, LEN, D), 1.0, 6.0, ((0, 8), (1, 4)))
    frames = set_ends(jax.random.randint(streams_of[1], (CLIPS,), F_MIN, F_MAX + 1), jax.random.fold_in(streams_of[1], 1), F_MIN, F_MAX).astype(jnp.int32)
    text_mask = set_ends((jax.random.randint(streams_of[2], (CLIPS, TXT), 0, 4) < 3).astype(jnp.int32), jax.random.fold_in(streams_of[2], 1), 0, 1)
    latents = noise(streams_of[3], (CLIPS, NL, D), 1.0, 6.0, ((0, 8),))
    cross_q = noise(streams_of[4], (D, D), D ** -0.5, 0.21875, ((0, 4),))
    cross_kv = noise(streams_of[5], (2, D, D), D ** -0.5, 0.21875, ((1, 4),))
    cross_out = noise(streams_of[6], (D, D), (max(D // 256, 1)) ** -0.5, 3.5, ((0, 4),))
    cross_up = noise(streams_of[7], (D, FF), D ** -0.5, 0.21875, ((1, 4),))
    cross_down = noise(streams_of[8], (FF, D), FF ** -0.5, 0.109375, ((0, 4),))
    self_qkv = noise(streams_of[9], (3, D, D), D ** -0.5, 0.21875, ((1, 4),))
    self_out = noise(streams_of[10], (D, D), (max(D // 16, 1)) ** -0.5, 0.875, ((0, 4),))
    self_up = noise(streams_of[11], (D, FF), D ** -0.5, 0.21875, ((1, 4),))
    self_down = noise(streams_of[12], (FF, D), FF ** -0.5, 0.109375, ((0, 4),))
    head_bias = noise(streams_of[13], (2, 2, D), 0.3, 1.8, ((2, 4),), jnp.float32)
    up_bias = noise(streams_of[14], (2, FF), 0.3, 1.8, ((1, 4),), jnp.float32)
    out_bias = noise(streams_of[15], (2, 2, D), 0.3, 1.8, (), jnp.float32)
    norm_gain = jnp.clip(1.0 + 0.1 * jax.random.normal(streams_of[16], (5, D), jnp.float32), 0.5, 1.5)
    norm_bias = noise(streams_of[17], (5, D), 0.3, 1.8, (), jnp.float32)
    latents_cot = noise(streams_of[18], (CLIPS, NL, D), 1.0, 6.0, ((0, 8),), jnp.float32)
    return {"tokens": tokens, "frames": frames, "text_mask": text_mask, "latents": latents, "cross_q": cross_q, "cross_kv": cross_kv, "cross_out": cross_out, "cross_up": cross_up, "cross_down": cross_down, "self_qkv": self_qkv, "self_out": self_out, "self_up": self_up, "self_down": self_down, "head_bias": head_bias, "up_bias": up_bias, "out_bias": out_bias, "norm_gain": norm_gain, "norm_bias": norm_bias, "latents_cot": latents_cot}


@jax.custom_vjp
def low(v):
    return lax.optimization_barrier(v.astype(jnp.bfloat16)).astype(jnp.float32)

@jax.custom_vjp
def low_back(v):
    return v

def low_keep(v):
    return (low(v), None)

def low_pass(kept, grad):
    return (grad,)

def back_keep(v):
    return (v, None)

def back_low(kept, grad):
    return (low(grad),)
low.defvjp(low_keep, low_pass)
low_back.defvjp(back_keep, back_low)

def both_ways(tensor):
    return low(low_back(tensor))

def product(left, right):
    return jnp.matmul(left, right, precision=lax.Precision.HIGHEST)

def normed(tensor, gain_row, shift_row):
    row_mean = lax.optimization_barrier(jnp.mean(tensor, axis=-1, keepdims=True))
    centered = tensor - row_mean
    spread = lax.optimization_barrier(jnp.mean(centered * centered, axis=-1, keepdims=True))
    return centered * lax.rsqrt(spread + 1e-05) * gain_row + shift_row

def attend(queries, key_rows, values, usable):
    query_count = queries.shape[0]
    key_count = key_rows.shape[0]
    queries = queries.reshape(query_count, HEADS, HD)
    key_rows = key_rows.reshape(key_count, HEADS, HD)
    values = values.reshape(key_count, HEADS, HD)
    scores = low_back(jnp.einsum('qhe,khe->hqk', queries, key_rows, precision=lax.Precision.HIGHEST))
    scores = jnp.where(usable[None, None, :], scores, -1e+30)
    row_max = lax.optimization_barrier(jnp.max(scores, axis=-1, keepdims=True))
    powers = jnp.exp(scores - row_max)
    chances = low(powers / lax.optimization_barrier(jnp.sum(powers, axis=-1, keepdims=True)))
    mixture = jnp.einsum('hqk,khe->qhe', chances, values, precision=lax.Precision.HIGHEST)
    return both_ways(mixture).reshape(query_count, HEADS * HD)

def feed_forward(tensor, gain_row, shift_row, weight_up, bias_up, weight_down):
    hidden = low(normed(tensor, gain_row, shift_row))
    pre_act = low_back(product(hidden, weight_up) + bias_up)
    activation = low(jax.nn.gelu(pre_act, approximate=True))
    return low_back(product(activation, weight_down))

def full_layer(params, clip_tokens, clip_latents, clip_usable):
    cross_q, cross_kv, cross_out, cross_up, cross_down, self_qkv, self_out, self_up, self_down, head_bias, up_bias, out_bias, norm_gain, norm_bias = params
    scaling = HD ** (-0.5)
    inputs = low(normed(clip_tokens, norm_gain[0], norm_bias[0]))
    latent_norm = low(normed(clip_latents, norm_gain[1], norm_bias[1]))
    queries = both_ways((product(latent_norm, cross_q.T) + head_bias[0, 0]) * scaling)
    key_rows = both_ways(product(inputs, cross_kv[0].T))
    values = both_ways(product(inputs, cross_kv[1].T) + head_bias[0, 1])
    mixture = attend(queries, key_rows, values, clip_usable)
    after_cross = clip_latents + low_back(product(mixture, cross_out)) + out_bias[0, 0]
    after_mlp = after_cross + feed_forward(after_cross, norm_gain[2], norm_bias[2], cross_up, up_bias[0], cross_down) + out_bias[0, 1]
    self_norm = low(normed(after_mlp, norm_gain[3], norm_bias[3]))
    queries = both_ways((product(self_norm, self_qkv[0].T) + head_bias[1, 0]) * scaling)
    key_rows = both_ways(product(self_norm, self_qkv[1].T))
    values = both_ways(product(self_norm, self_qkv[2].T) + head_bias[1, 1])
    everyone = jnp.ones((self_norm.shape[0],), dtype=bool)
    mixture = attend(queries, key_rows, values, everyone)
    after_self = after_mlp + low_back(product(mixture, self_out)) + out_bias[1, 0]
    return after_self + feed_forward(after_self, norm_gain[4], norm_bias[4], self_up, up_bias[1], self_down) + out_bias[1, 1]

def reference(tokens, frames, text_mask, latents, cross_q, cross_kv, cross_out, cross_up, cross_down, self_qkv, self_out, self_up, self_down, head_bias, up_bias, out_bias, norm_gain, norm_bias, latents_cot):
    params = tuple((weight.astype(jnp.float32) for weight in (cross_q, cross_kv, cross_out, cross_up, cross_down, self_qkv, self_out, self_up, self_down, head_bias, up_bias, out_bias, norm_gain, norm_bias)))
    position = jnp.arange(LEN, dtype=jnp.int32)
    text_full = jnp.concatenate([jnp.zeros((CLIPS, F_MAX * P_SIZE), jnp.int32), text_mask], axis=1)
    usable = (position[None, :] < frames[:, None] * P_SIZE) | (text_full == 1)

    def forward(weights, all_tokens, all_latents):

        def one_clip(clip_arrays):
            return full_layer(weights, clip_arrays[0], clip_arrays[1], clip_arrays[2])
        return lax.map(jax.checkpoint(one_clip), (all_tokens, all_latents, usable))
    result, pullback = jax.vjp(forward, params, tokens.astype(jnp.float32), latents.astype(jnp.float32))
    gradients, token_grad, latent_grad = pullback(latents_cot)
    return (result, token_grad.astype(jnp.bfloat16), latent_grad, gradients[0], gradients[1], gradients[2], gradients[3], gradients[4], gradients[5], gradients[6], gradients[7], gradients[8], gradients[9], gradients[10], gradients[11], gradients[12], gradients[13])
```

```python
from functools import partial

import jax
import jax.numpy as jnp
from jax import lax
from jax.sharding import PartitionSpec as P

HD = 64
P_SIZE = 392
F_MAX = 16


EPSILON = 1e-05
NEGATIVE = -1e30


def normed(tensor, gain_row, shift_row):
    row_mean = jnp.mean(tensor, axis=-1, keepdims=True)
    centered = tensor - row_mean
    spread = jnp.mean(centered * centered, axis=-1, keepdims=True)
    return centered * lax.rsqrt(spread + EPSILON) * gain_row + shift_row


def share_of(tensor, head_index, head_width):
    return lax.dynamic_slice_in_dim(tensor, head_index * head_width, head_width, tensor.ndim - 1)


def split_heads(tensor, heads_here):
    return tensor.reshape(
        tensor.shape[0], tensor.shape[1], heads_here, tensor.shape[2] // heads_here
    )


def merge_heads(tensor):
    return tensor.reshape(tensor.shape[0], tensor.shape[1], tensor.shape[2] * tensor.shape[3])


def join_heads(partial_sum):
    return lax.psum(partial_sum.astype(jnp.bfloat16), "head").astype(jnp.float32)


def join_back(partial_sum):
    return lax.psum(partial_sum.astype(jnp.bfloat16), "head").astype(jnp.float32)


def scores_of(queries, key_rows, usable):
    scores = jnp.einsum("qhe,khe->hqk", queries, key_rows, preferred_element_type=jnp.float32)
    return jnp.where(usable[None, None, :], scores, NEGATIVE)


def attend_parts(parts):
    queries, key_rows, values, usable = parts
    scores = scores_of(queries, key_rows, usable)
    row_max = jnp.max(scores, axis=-1, keepdims=True)
    powers = jnp.exp(scores - row_max)
    totals = jnp.sum(powers, axis=-1, keepdims=True)
    chances = (powers / totals).astype(jnp.bfloat16)
    mixture = jnp.einsum("hqk,khe->qhe", chances, values, preferred_element_type=jnp.float32)
    return (mixture.astype(jnp.bfloat16), row_max, totals)


def back_parts(parts):
    queries, key_rows, values, usable, row_max, totals, grad_mix = parts
    scores = scores_of(queries, key_rows, usable)
    chances = jnp.exp(scores - row_max) / totals
    rounded = chances.astype(jnp.bfloat16)
    grad_values = jnp.einsum(
        "hqk,qhe->khe", rounded, grad_mix, preferred_element_type=jnp.float32
    ).astype(jnp.bfloat16)
    grad_chances = jnp.einsum("qhe,khe->hqk", grad_mix, values, preferred_element_type=jnp.float32)
    inner_sum = jnp.sum(chances * grad_chances, axis=-1, keepdims=True)
    grad_scores = (chances * (grad_chances - inner_sum)).astype(jnp.bfloat16)
    grad_queries = jnp.einsum(
        "hqk,khe->qhe", grad_scores, key_rows, preferred_element_type=jnp.float32
    ).astype(jnp.bfloat16)
    grad_keys = jnp.einsum(
        "hqk,qhe->khe", grad_scores, queries, preferred_element_type=jnp.float32
    ).astype(jnp.bfloat16)
    return (grad_queries, grad_keys, grad_values)


def feed_forward(tensor, gain_row, shift_row, weight_up, bias_up, weight_down):
    hidden = normed(tensor, gain_row, shift_row).astype(jnp.bfloat16)
    pre_act = (
        jnp.einsum("cnd,df->cnf", hidden, weight_up, preferred_element_type=jnp.float32) + bias_up
    )
    activation = jax.nn.gelu(pre_act, approximate=True).astype(jnp.bfloat16)
    partial_sum = jnp.einsum(
        "cnf,fd->cnd", activation, weight_down, preferred_element_type=jnp.float32
    )
    return (join_heads(partial_sum), (hidden, pre_act, activation))


def feed_back(tensor, gain_row, shift_row, weight_up, weight_down, saved_acts, grad_out):
    hidden, pre_act, activation = saved_acts
    grad_branch = grad_out.astype(jnp.bfloat16)
    grad_weight_down = jnp.einsum(
        "cnf,cnd->fd", activation, grad_branch, preferred_element_type=jnp.float32
    )
    grad_act = jnp.einsum(
        "cnd,fd->cnf", grad_branch, weight_down, preferred_element_type=jnp.float32
    )
    unused, gelu_pull = jax.vjp(partial(jax.nn.gelu, approximate=True), pre_act)
    grad_pre = gelu_pull(grad_act)[0].astype(jnp.bfloat16)
    grad_weight_up = jnp.einsum("cnd,cnf->df", hidden, grad_pre, preferred_element_type=jnp.float32)
    grad_bias_up = jnp.sum(grad_pre.astype(jnp.float32), axis=(0, 1))
    grad_hidden = join_back(
        jnp.einsum("cnf,df->cnd", grad_pre, weight_up, preferred_element_type=jnp.float32)
    )
    unused_too, norm_pull = jax.vjp(normed, tensor, gain_row, shift_row)
    grad_tensor, grad_gain, grad_shift = norm_pull(grad_hidden)
    return (grad_tensor, grad_weight_up, grad_bias_up, grad_weight_down, grad_gain, grad_shift)


def local(
    tokens,
    frames,
    text_mask,
    latents,
    cross_q,
    cross_kv,
    cross_out,
    cross_up,
    cross_down,
    self_qkv,
    self_out,
    self_up,
    self_down,
    head_bias,
    up_bias,
    out_bias,
    norm_gain,
    norm_bias,
    latents_cot,
):
    head_index = lax.axis_index("head")
    head_width = cross_q.shape[0]
    heads_here = head_width // HD
    scaling = HD ** (-0.5)
    clips_here = tokens.shape[0]
    rows_here = tokens.shape[1]
    length = rows_here * lax.axis_size("head")
    position = jnp.arange(length, dtype=jnp.int32)
    text_full = jnp.concatenate(
        [jnp.zeros((clips_here, F_MAX * P_SIZE), jnp.int32), text_mask], axis=1
    )
    usable = (position[None, :] < frames[:, None] * P_SIZE) | (text_full == 1)
    gathered, weights_whole = (
        lax.all_gather(tokens, "head", axis=1, tiled=True),
        lax.all_gather(cross_kv, "head", axis=1, tiled=True),
    )
    full_rows = gathered.astype(jnp.float32)
    row_mean = jnp.mean(full_rows, axis=-1, keepdims=True)
    centered = full_rows - row_mean
    inverse = lax.rsqrt(jnp.mean(centered * centered, axis=-1, keepdims=True) + EPSILON)
    inputs = (centered * inverse * norm_gain[0] + norm_bias[0]).astype(jnp.bfloat16)
    key_value = jnp.einsum("cld,kwd->clkw", inputs, cross_kv, preferred_element_type=jnp.float32)
    key_rows = key_value[:, :, 0].astype(jnp.bfloat16)
    cross_values = (key_value[:, :, 1] + head_bias[0, 1]).astype(jnp.bfloat16)
    start_state = latents.astype(jnp.float32)
    latent_norm = normed(start_state, norm_gain[1], norm_bias[1]).astype(jnp.bfloat16)
    cross_queries = (
        (
            jnp.einsum("cnd,wd->cnw", latent_norm, cross_q, preferred_element_type=jnp.float32)
            + head_bias[0, 0]
        )
        * scaling
    ).astype(jnp.bfloat16)
    cross_parts = (
        split_heads(cross_queries, heads_here),
        split_heads(key_rows, heads_here),
        split_heads(cross_values, heads_here),
        usable,
    )
    cross_mix, cross_max, cross_totals = lax.map(attend_parts, cross_parts)
    cross_flat = merge_heads(cross_mix)
    after_cross = (
        start_state
        + join_heads(
            jnp.einsum("cnw,wd->cnd", cross_flat, cross_out, preferred_element_type=jnp.float32)
        )
        + out_bias[0, 0]
    )
    cross_branch, cross_saved = feed_forward(
        after_cross, norm_gain[2], norm_bias[2], cross_up, up_bias[0], cross_down
    )
    after_mlp = after_cross + cross_branch + out_bias[0, 1]
    self_norm = normed(after_mlp, norm_gain[3], norm_bias[3]).astype(jnp.bfloat16)
    triple = jnp.einsum("cnd,kwd->cnkw", self_norm, self_qkv, preferred_element_type=jnp.float32)
    self_queries = ((triple[:, :, 0] + head_bias[1, 0]) * scaling).astype(jnp.bfloat16)
    self_keys = triple[:, :, 1].astype(jnp.bfloat16)
    self_values = (triple[:, :, 2] + head_bias[1, 1]).astype(jnp.bfloat16)
    everyone = jnp.ones((clips_here, self_keys.shape[1]), dtype=bool)
    self_parts = (
        split_heads(self_queries, heads_here),
        split_heads(self_keys, heads_here),
        split_heads(self_values, heads_here),
        everyone,
    )
    self_mix, self_max, self_totals = lax.map(attend_parts, self_parts)
    self_flat = merge_heads(self_mix)
    after_self = (
        after_mlp
        + join_heads(
            jnp.einsum("cnw,wd->cnd", self_flat, self_out, preferred_element_type=jnp.float32)
        )
        + out_bias[1, 0]
    )
    self_branch, self_saved = feed_forward(
        after_self, norm_gain[4], norm_bias[4], self_up, up_bias[1], self_down
    )
    latents_out = after_self + self_branch + out_bias[1, 1]
    bias_self_mlp = jnp.sum(latents_cot, axis=(0, 1))
    grad_ln_four, grad_self_up, upbias_self, grad_self_down, gain_four, shift_four = feed_back(
        after_self, norm_gain[4], norm_bias[4], self_up, self_down, self_saved, latents_cot
    )
    grad_state = latents_cot + grad_ln_four
    bias_self_attn = jnp.sum(grad_state, axis=(0, 1))
    grad_attn_in = grad_state.astype(jnp.bfloat16)
    grad_self_out = jnp.einsum(
        "cnw,cnd->wd", self_flat, grad_attn_in, preferred_element_type=jnp.float32
    )
    grad_mix = jnp.einsum(
        "cnd,wd->cnw", grad_attn_in, self_out, preferred_element_type=jnp.float32
    ).astype(jnp.bfloat16)
    self_grads = lax.map(
        back_parts, self_parts + (self_max, self_totals, split_heads(grad_mix, heads_here))
    )
    grad_query_scaled = (merge_heads(self_grads[0]).astype(jnp.float32) * scaling).astype(
        jnp.bfloat16
    )
    grad_triple = jnp.stack(
        [grad_query_scaled, merge_heads(self_grads[1]), merge_heads(self_grads[2])], axis=2
    )
    grad_self_qkv = jnp.einsum(
        "cnd,cnkw->kwd", self_norm, grad_triple, preferred_element_type=jnp.float32
    )
    bias_self_q = jnp.sum(grad_triple[:, :, 0].astype(jnp.float32), axis=(0, 1))
    bias_self_v = jnp.sum(grad_triple[:, :, 2].astype(jnp.float32), axis=(0, 1))
    grad_self_in = join_back(
        jnp.einsum("cnkw,kwd->cnd", grad_triple, self_qkv, preferred_element_type=jnp.float32)
    )
    unused, norm_pull = jax.vjp(normed, after_mlp, norm_gain[3], norm_bias[3])
    grad_ln_three, gain_three, shift_three = norm_pull(grad_self_in)
    grad_state = grad_state + grad_ln_three
    bias_cross_mlp = jnp.sum(grad_state, axis=(0, 1))
    grad_ln_two, grad_cross_up, upbias_cross, grad_cross_down, gain_two, shift_two = feed_back(
        after_cross, norm_gain[2], norm_bias[2], cross_up, cross_down, cross_saved, grad_state
    )
    grad_state = grad_state + grad_ln_two
    bias_cross_attn = jnp.sum(grad_state, axis=(0, 1))
    grad_attn_in = grad_state.astype(jnp.bfloat16)
    grad_cross_out = jnp.einsum(
        "cnw,cnd->wd", cross_flat, grad_attn_in, preferred_element_type=jnp.float32
    )
    grad_mix = jnp.einsum(
        "cnd,wd->cnw", grad_attn_in, cross_out, preferred_element_type=jnp.float32
    ).astype(jnp.bfloat16)
    cross_grads = lax.map(
        back_parts, cross_parts + (cross_max, cross_totals, split_heads(grad_mix, heads_here))
    )
    grad_query_cross = (merge_heads(cross_grads[0]).astype(jnp.float32) * scaling).astype(
        jnp.bfloat16
    )
    grad_cross_q = jnp.einsum(
        "cnd,cnw->wd", latent_norm, grad_query_cross, preferred_element_type=jnp.float32
    )
    bias_cross_q = jnp.sum(grad_query_cross.astype(jnp.float32), axis=(0, 1))
    grad_latent_in = join_back(
        jnp.einsum("cnw,wd->cnd", grad_query_cross, cross_q, preferred_element_type=jnp.float32)
    )
    unused_too, latent_pull = jax.vjp(normed, start_state, norm_gain[1], norm_bias[1])
    grad_ln_one, gain_one, shift_one = latent_pull(grad_latent_in)
    grad_latents = grad_state + grad_ln_one
    grad_pair = jnp.stack([merge_heads(cross_grads[1]), merge_heads(cross_grads[2])], axis=2)
    grad_cross_kv = jnp.einsum(
        "cld,clkw->kwd", inputs, grad_pair, preferred_element_type=jnp.float32
    )
    bias_cross_v = jnp.sum(grad_pair[:, :, 1].astype(jnp.float32), axis=(0, 1))
    arrived = lax.all_to_all(grad_pair, "head", split_axis=1, concat_axis=3, tiled=True)
    grad_share = jnp.einsum(
        "clkw,kwd->cld", arrived, weights_whole, preferred_element_type=jnp.float32
    )
    own_start = head_index * rows_here
    own_mean = lax.dynamic_slice_in_dim(row_mean, own_start, rows_here, 1)
    own_inverse = lax.dynamic_slice_in_dim(inverse, own_start, rows_here, 1)
    standard = (tokens.astype(jnp.float32) - own_mean) * own_inverse
    scaled = grad_share * norm_gain[0]
    mean_plain = jnp.mean(scaled, axis=-1, keepdims=True)
    mean_cross = jnp.mean(scaled * standard, axis=-1, keepdims=True)
    grad_tokens = (own_inverse * (scaled - mean_plain - standard * mean_cross)).astype(jnp.bfloat16)
    gain_zero, shift_zero = lax.psum(
        (jnp.sum(grad_share * standard, axis=(0, 1)), jnp.sum(grad_share, axis=(0, 1))), "head"
    )
    grad_head_bias = jnp.stack(
        [jnp.stack([bias_cross_q, bias_cross_v]), jnp.stack([bias_self_q, bias_self_v])]
    )
    grad_up_bias = jnp.stack([upbias_cross, upbias_self])
    out_full = jnp.stack(
        [jnp.stack([bias_cross_attn, bias_cross_mlp]), jnp.stack([bias_self_attn, bias_self_mlp])]
    )
    grad_out_bias = share_of(out_full, head_index, head_width)
    grad_norm_gain = share_of(
        jnp.stack([gain_zero, gain_one, gain_two, gain_three, gain_four]), head_index, head_width
    )
    grad_norm_bias = share_of(
        jnp.stack([shift_zero, shift_one, shift_two, shift_three, shift_four]),
        head_index,
        head_width,
    )
    small_sums = lax.psum(
        (grad_head_bias, grad_up_bias, grad_out_bias, grad_norm_gain, grad_norm_bias), "dp"
    )
    pieces = [
        grad_cross_q.T,
        grad_cross_kv[0].T,
        grad_cross_kv[1].T,
        grad_cross_out.T,
        grad_self_qkv[0].T,
        grad_self_qkv[1].T,
        grad_self_qkv[2].T,
        grad_self_out.T,
        grad_cross_up,
        grad_cross_down.T,
        grad_self_up,
        grad_self_down.T,
    ]
    packed = jnp.concatenate([piece.astype(jnp.bfloat16) for piece in pieces], axis=1)
    summed = lax.psum_scatter(packed, "dp", scatter_dimension=0, tiled=True).astype(jnp.float32)
    sums = []
    start = 0
    for piece in pieces:
        sums.append(summed[:, start : start + piece.shape[1]])
        start += piece.shape[1]
    return (
        latents_out,
        grad_tokens,
        grad_latents,
        sums[0].T,
        jnp.stack([sums[1].T, sums[2].T]),
        sums[3].T,
        sums[8],
        sums[9].T,
        jnp.stack([sums[4].T, sums[5].T, sums[6].T]),
        sums[7].T,
        sums[10],
        sums[11].T,
        small_sums[0],
        small_sums[1],
        small_sums[2],
        small_sums[3],
        small_sums[4],
    )


def solution(mesh):
    in_specs = (
        P("dp", "head", None),
        P("dp"),
        P("dp", None),
        P("dp", None, None),
        P("head", None),
        P(None, "head", None),
        P("head", None),
        P(None, "head"),
        P("head", None),
        P(None, "head", None),
        P("head", None),
        P(None, "head"),
        P("head", None),
        P(None, None, "head"),
        P(None, "head"),
        P(),
        P(),
        P(),
        P("dp", None, None),
    )
    out_specs = (
        P("dp", None, None),
        P("dp", "head", None),
        P("dp", None, None),
        P("head", "dp"),
        P(None, "head", "dp"),
        P("head", "dp"),
        P("dp", "head"),
        P("head", "dp"),
        P(None, "head", "dp"),
        P("head", "dp"),
        P("dp", "head"),
        P("head", "dp"),
        P(None, None, "head"),
        P(None, "head"),
        P(None, None, "head"),
        P(None, "head"),
        P(None, "head"),
    )
    return jax.shard_map(local, mesh=mesh, in_specs=in_specs, out_specs=out_specs, check_vma=False)
```
